32 devices in a mesh: grp: 4 (over y, x), row: 8 (over z, core).
Axes of the slice: x: 2, y: 2, z: 4, core: 2. Of those that a mesh axis runs over, the one named last changes fastest.
Arguments:
- a_tiles: bfloat16 [64, 4, 7, 128, 128], P('row', 'grp'), may hold values from -0.5 to 0.5
- a_cols: int32 [64, 4, 7], P('row', 'grp'), may hold values from 0 to 63, as said below
- p_tiles: bfloat16 [64, 4, 128, 128], P('row'), may hold values from -0.5 to 0.5
- p_cols: int32 [64, 4], replicated, may hold values from 0 to 31, as said below
- c_cols: int32 [32, 16], replicated, may hold values from 0 to 31, as said below
Outputs:
- coarse: float32 [32, 16, 128, 128], P('row', 'grp')
The draws below stay inside these ranges and needn't reach their ends.
Inputs may be any that keep to these rules, and one draw needn't show every extreme that they name: For fine tile row i in block b = i // 8, every entry of a_cols[i] lies in [max(b - 2, 0) * 8, min(b + 3, 8) * 8). For fine tile row i in block b = i // 8, the entries of p_cols[i] are distinct and lie in [(b - 1) * 4, (b + 2) * 4). For coarse tile row c in block t = c // 4, the entries of c_cols[c] are distinct and lie among the 20 coarse tile rows that start at min(max(t - 2, 0), 3) * 4.
All inputs are finite; a program needn't handle non-finite values.
Results may differ from the reference program's by a relative error of at most 0.0003.
Values may be sent and summed in bfloat16 or wider, within the bound.
A program may use at most 128 MiB of HBM per device.

```python
import jax
import jax.numpy as jnp
from jax import lax

TILE = 128
CT_DEV = 4
SLOTS = 7
KP = 4
KC = 16
FT_DEV = 8
GROUPS = 4
FT = 64
NCT = 32


def pick_distinct(key, count, width, valid, take):
    offsets = jnp.arange(width, dtype=jnp.int32)[None, :]
    scores = jax.random.randint(key, (count, width), 0, 1 << 20, dtype=jnp.int32) * width + offsets
    scores = jnp.where(valid, scores, -1 - offsets)
    top_scores, chosen = lax.top_k(scores, take)
    return chosen.astype(jnp.int32)


def draw_a_cols(key, part):
    fine_ids = jnp.arange(FT, dtype=jnp.int32)
    owner = fine_ids // FT_DEV
    lowest = jnp.maximum(owner - 2, 0) * FT_DEV
    highest_row = jnp.minimum(owner + 3, FT // FT_DEV) * FT_DEV
    spans = (highest_row - lowest)[:, None, None]
    picks = jax.random.randint(jax.random.fold_in(key, 17), (FT, GROUPS, SLOTS), 0, 1 << 30, dtype=jnp.int32)
    return (lowest[:, None, None] + picks % spans).astype(jnp.int32)


def draw_p_cols(key, part):
    fine_ids = jnp.arange(FT, dtype=jnp.int32)
    owner = fine_ids // FT_DEV
    begin = (owner - 1) * CT_DEV
    candidate = begin[:, None] + jnp.arange(3 * CT_DEV, dtype=jnp.int32)[None, :]
    valid = (candidate >= 0) & (candidate < NCT)
    chosen = pick_distinct(jax.random.fold_in(key, 29), FT, 3 * CT_DEV, valid, KP)
    return (begin[:, None] + chosen).astype(jnp.int32)


def draw_c_cols(key, part):
    coarse_ids = jnp.arange(NCT, dtype=jnp.int32)
    owner = coarse_ids // CT_DEV
    begin = jnp.clip(owner - 2, 0, NCT // CT_DEV - 5) * CT_DEV
    valid = jnp.ones((NCT, 5 * CT_DEV), dtype=bool)
    chosen = pick_distinct(jax.random.fold_in(key, 41), NCT, 5 * CT_DEV, valid, KC)
    return (begin[:, None] + chosen).astype(jnp.int32)


def block_levels(own_key, dims, pieces, least, high):
    gain = 1.0
    for axis_at, blocks in pieces:
        draws = jax.random.uniform(jax.random.fold_in(jax.random.fold_in(own_key, 6), axis_at), (blocks,), jnp.float32, least / len(pieces), high / len(pieces))
        gain = gain * jnp.repeat(jnp.exp(draws), dims[axis_at] // blocks).reshape((-1,) + (1,) * (len(dims) - 1 - axis_at))
    return gain


def normal_values(rng, dims, scale, bound, split=(), kind=jnp.bfloat16):
    loudness = block_levels(rng, dims, split, -0.22, 0.18) if split else 1.0
    entries = jax.random.normal(rng, dims, jnp.float32) * scale * loudness
    return jnp.minimum(jnp.maximum(entries, -bound), bound).astype(kind)


def setup_inputs(seed: int = 0) -> dict:
    splits = jax.random.split(jax.random.key(seed), 6)
    a_tiles = normal_values(splits[0], (FT, GROUPS, SLOTS, TILE, TILE), TILE ** -0.5, 0.5, ((0, 8), (1, 4)))
    a_cols = draw_a_cols(jax.random.fold_in(splits[5], 71), 0)
    p_tiles = normal_values(splits[2], (FT, KP, TILE, TILE), TILE ** -0.5, 0.5, ((0, 8),))
    p_cols = draw_p_cols(jax.random.fold_in(splits[5], 71), 0)
    c_cols = draw_c_cols(jax.random.fold_in(splits[5], 71), 0)
    return dict(a_tiles=a_tiles, a_cols=a_cols, p_tiles=p_tiles, p_cols=p_cols, c_cols=c_cols)


highest = lax.Precision.HIGHEST


def reference(a_tiles, a_cols, p_tiles, p_cols, c_cols):
    def fine_row(coarse, inputs):
        a_row, columns, own_tiles, own_cols = inputs
        targets = c_cols[own_cols]
        fetched = p_tiles[columns].astype(jnp.float32)
        fetched_cols = p_cols[columns]
        products = jnp.einsum("gsxy,gspyz->gspxz", a_row.astype(jnp.float32), fetched, precision=highest)
        matches = (fetched_cols[:, :, :, None, None] == targets[None, None, None, :, :]).astype(jnp.float32)
        partial_value = jnp.einsum("gspxz,gspqk->gqkxz", products, matches, precision=highest)
        summed = jnp.sum(partial_value, axis=0)
        row_terms = jnp.einsum("qyx,qkyz->qkxz", own_tiles.astype(jnp.float32), summed, precision=highest)
        return coarse.at[own_cols].add(row_terms), None

    initial = jnp.zeros((NCT, KC, TILE, TILE), jnp.float32)
    result = lax.scan(fine_row, initial, (a_tiles, a_cols, p_tiles, p_cols))[0]
    return result
```

```python
import functools

import jax
import jax.numpy as jnp
from jax import lax
from jax.experimental import pallas as pl
from jax.experimental.pallas import tpu as pltpu
from jax.sharding import PartitionSpec as P

RATIO = 2
REACH = 2


def passed_along(x, axis, by):
    size = lax.axis_size(axis)
    pairs = [(i, i + by) for i in range(size) if 0 <= i + by < size]
    return lax.ppermute(x, axis, pairs)


def product_kernel(
    sizes, where, a_cols, p_cols, c_cols, a_ref, band_ref, total_ref, spread, halves
):
    fine_rows, slots, kp, kc, tile = sizes
    coarse_rows = fine_rows // RATIO
    window = (2 * (REACH + 1) + 1) * coarse_rows
    position = where[0]
    first_row = position * fine_rows
    band_start = first_row - REACH * fine_rows
    window_start = (position - REACH - 1) * coarse_rows
    base_coarse = (position - 1) * coarse_rows
    total_ref[...] = jnp.zeros_like(total_ref)
    halves[window] = jnp.zeros((2 * tile, tile), jnp.bfloat16)
    group = min(4, kc)

    @pl.loop(0, fine_rows)
    def _(i):
        spread[...] = jnp.zeros_like(spread)
        for s in range(slots):
            j = a_cols[i * slots + s]
            local = (j - band_start) * kp
            right = jnp.concatenate([band_ref[local + p] for p in range(kp)], axis=1)
            prod = jnp.dot(a_ref[i * slots + s], right, preferred_element_type=jnp.float32)
            for p in range(kp):
                w = p_cols[j * kp + p] - window_start
                spread[w] = spread[w] + prod[:, p * tile : (p + 1) * tile]

        @pl.loop(0, window, unroll=4)
        def _(w):
            value = spread[w]
            high = value.astype(jnp.bfloat16)
            halves[w, :tile] = high
            halves[w, tile:] = (value - high.astype(jnp.float32)).astype(jnp.bfloat16)

        for q in range(kp):
            c = p_cols[(first_row + i) * kp + q]
            own = band_ref[(REACH * fine_rows + i) * kp + q].T
            left = jnp.concatenate([own, own], axis=1)
            out = (c - base_coarse) * kc
            for k in range(0, kc, group):
                parts = []
                for n in range(group):
                    w = c_cols[c * kc + k + n] - window_start
                    w = jnp.where((w < 0) | (w >= window), window, w)
                    parts.append(halves[w])
                prod = jnp.dot(
                    left, jnp.concatenate(parts, axis=1), preferred_element_type=jnp.float32
                )
                for n in range(group):
                    at = out + k + n
                    total_ref[at] = total_ref[at] + prod[:, n * tile : (n + 1) * tile]


def local_products(a_tiles, a_cols, band, p_cols, c_cols, position):
    fine_rows, _, slots, tile, _ = a_tiles.shape
    kp = band.shape[1]
    kc = c_cols.shape[1]
    coarse_rows = fine_rows // RATIO
    window = (2 * (REACH + 1) + 1) * coarse_rows
    smem = pl.BlockSpec(memory_space=pltpu.SMEM)
    vmem = pl.BlockSpec(memory_space=pltpu.VMEM)
    return pl.pallas_call(
        functools.partial(product_kernel, (fine_rows, slots, kp, kc, tile)),
        out_shape=jax.ShapeDtypeStruct((3 * coarse_rows * kc, tile, tile), jnp.float32),
        in_specs=[smem] * 4 + [vmem] * 2,
        out_specs=vmem,
        scratch_shapes=[
            pltpu.VMEM((window, tile, tile), jnp.float32),
            pltpu.VMEM((window + 1, 2 * tile, tile), jnp.bfloat16),
        ],
        compiler_params=pltpu.CompilerParams(vmem_limit_bytes=56 * 1024 * 1024),
    )(
        position.reshape(1),
        a_cols.reshape(-1),
        p_cols.reshape(-1),
        c_cols.reshape(-1),
        a_tiles.reshape(-1, tile, tile),
        band.reshape(-1, tile, tile),
    )


def body(a_tiles, a_cols, p_tiles, p_cols, c_cols):
    fine_rows = a_tiles.shape[0]
    coarse_rows = fine_rows // RATIO
    tile = a_tiles.shape[-1]
    kc = c_cols.shape[1]
    position = lax.axis_index("row")
    fetched = [passed_along(p_tiles, "row", offset) for offset in (2, 1, -1, -2)]
    band = jnp.concatenate([fetched[0], fetched[1], p_tiles, fetched[2], fetched[3]], axis=0)
    total = local_products(a_tiles, a_cols, band, p_cols, c_cols, position)
    total = total.reshape(3, coarse_rows, kc, tile, tile)
    center = total[1] + passed_along(total[0], "row", -1) + passed_along(total[2], "row", 1)
    return lax.psum_scatter(center, "grp", scatter_dimension=1, tiled=True)


def solution(mesh):
    return jax.shard_map(
        body,
        mesh=mesh,
        in_specs=(
            P("row", "grp", None, None, None),
            P("row", "grp", None),
            P("row", None, None, None),
            P(),
            P(),
        ),
        out_specs=P("row", "grp", None, None),
        check_vma=False,
    )
```

```python
import functools

import jax
import jax.numpy as jnp
from jax import lax
from jax.experimental import pallas as pl
from jax.experimental.pallas import tpu as pltpu
from jax.sharding import PartitionSpec as P

RATIO = 2
REACH = 2


def passed_along(x, axis, by):
    size = lax.axis_size(axis)
    pairs = [(i, i + by) for i in range(size) if 0 <= i + by < size]
    return lax.ppermute(x, axis, pairs)


LEVELS = 32767.0


def encoded(value):
    most = jnp.maximum(jnp.max(jnp.abs(value), axis=0, keepdims=True), 2e-34)
    code = jnp.round(value * (LEVELS / most)).astype(jnp.int32).astype(jnp.int16)
    return code, most * (1.0 / LEVELS)


def decoded(code, scale):
    return code.astype(jnp.int32).astype(jnp.float32) * scale


def product_kernel(
    sizes,
    where,
    a_cols,
    p_cols,
    c_cols,
    a_ref,
    band_ref,
    center_ref,
    codes_ref,
    scales_ref,
    total_ref,
    spread,
    halves,
):
    fine_rows, slots, kp, kc, tile, chunks = sizes
    coarse_rows = fine_rows // RATIO
    window = (2 * (REACH + 1) + 1) * coarse_rows
    position = where[0]
    first_row = position * fine_rows
    band_start = first_row - REACH * fine_rows
    window_start = (position - REACH - 1) * coarse_rows
    base_coarse = (position - 1) * coarse_rows
    total_ref[...] = jnp.zeros_like(total_ref)
    halves[window] = jnp.zeros((2 * tile, tile), jnp.bfloat16)
    group = min(4, kc)

    @pl.loop(0, fine_rows)
    def _(i):
        spread[...] = jnp.zeros_like(spread)
        for s in range(slots):
            j = a_cols[i * slots + s]
            local = (j - band_start) * kp
            right = jnp.concatenate([band_ref[local + p] for p in range(kp)], axis=1)
            prod = jnp.dot(a_ref[i * slots + s], right, preferred_element_type=jnp.float32)
            for p in range(kp):
                w = p_cols[j * kp + p] - window_start
                spread[w] = spread[w] + prod[:, p * tile : (p + 1) * tile]

        @pl.loop(0, window, unroll=4)
        def _(w):
            value = spread[w]
            high = value.astype(jnp.bfloat16)
            halves[w, :tile] = high
            halves[w, tile:] = (value - high.astype(jnp.float32)).astype(jnp.bfloat16)

        for q in range(kp):
            c = p_cols[(first_row + i) * kp + q]
            own = band_ref[(REACH * fine_rows + i) * kp + q].T
            left = jnp.concatenate([own, own], axis=1)
            out = (c - base_coarse) * kc
            for k in range(0, kc, group):
                parts = []
                for n in range(group):
                    w = c_cols[c * kc + k + n] - window_start
                    w = jnp.where((w < 0) | (w >= window), window, w)
                    parts.append(halves[w])
                prod = jnp.dot(
                    left, jnp.concatenate(parts, axis=1), preferred_element_type=jnp.float32
                )
                for n in range(group):
                    at = out + k + n
                    total_ref[at] = total_ref[at] + prod[:, n * tile : (n + 1) * tile]

    share = kc // chunks
    for chunk in range(chunks):

        @pl.loop(0, coarse_rows)
        def _(c):
            for n in range(share):
                e = c * share + n
                k = chunk * share + n
                center_ref[chunk, e] = total_ref[(coarse_rows + c) * kc + k]
                for side in range(2):
                    value = total_ref[(2 * side * coarse_rows + c) * kc + k]
                    code, scale = encoded(value)
                    codes_ref[side, chunk, e] = code
                    scales_ref[side, chunk, pl.ds(e, 1)] = scale


def local_products(a_tiles, a_cols, band, p_cols, c_cols, position, chunks):
    fine_rows, _, slots, tile, _ = a_tiles.shape
    kp = band.shape[1]
    kc = c_cols.shape[1]
    coarse_rows = fine_rows // RATIO
    window = (2 * (REACH + 1) + 1) * coarse_rows
    members = coarse_rows * kc // chunks
    smem = pl.BlockSpec(memory_space=pltpu.SMEM)
    vmem = pl.BlockSpec(memory_space=pltpu.VMEM)
    return pl.pallas_call(
        functools.partial(product_kernel, (fine_rows, slots, kp, kc, tile, chunks)),
        out_shape=[
            jax.ShapeDtypeStruct((chunks, members, tile, tile), jnp.float32),
            jax.ShapeDtypeStruct((2, chunks, members, tile, tile), jnp.int16),
            jax.ShapeDtypeStruct((2, chunks, members, tile), jnp.float32),
        ],
        in_specs=[smem] * 4 + [vmem] * 2,
        out_specs=[vmem] * 3,
        scratch_shapes=[
            pltpu.VMEM((3 * coarse_rows * kc, tile, tile), jnp.float32),
            pltpu.VMEM((window, tile, tile), jnp.float32),
            pltpu.VMEM((window + 1, 2 * tile, tile), jnp.bfloat16),
        ],
        compiler_params=pltpu.CompilerParams(vmem_limit_bytes=56 * 1024 * 1024),
    )(
        position.reshape(1),
        a_cols.reshape(-1),
        p_cols.reshape(-1),
        c_cols.reshape(-1),
        a_tiles.reshape(-1, tile, tile),
        band.reshape(-1, tile, tile),
    )


def exchange_kernel(
    rows,
    chunks,
    center,
    codes,
    scales,
    out,
    side_codes,
    side_scales,
    sent_codes,
    sent_scales,
    peer_codes,
    peer_scales,
    side_sems,
    side_scale_sems,
    peer_sems,
    peer_scale_sems,
):
    r = lax.axis_index("row")
    g = lax.axis_index("grp")
    members = out.shape[0]
    barrier = pltpu.get_barrier_semaphore()
    mesh_type = pl.DeviceIdType.MESH

    def signal(where):
        pl.semaphore_signal(barrier, inc=1, device_id=where, device_id_type=mesh_type)

    for t in range(chunks - 1):
        signal({"grp": lax.rem(g + 1 + t, chunks)})

    @pl.when(r > 0)
    def _():
        signal({"row": r - 1})

    @pl.when(r < rows - 1)
    def _():
        signal({"row": r + 1})

    inside = (r > 0) & (r < rows - 1)

    @pl.when(inside)
    def _():
        pl.semaphore_wait(barrier, chunks + 1)

    @pl.when(jnp.logical_not(inside))
    def _():
        pl.semaphore_wait(barrier, chunks)

    sends = ((r > 0, r - 1), (r < rows - 1, r + 1))
    comes = (r < rows - 1, r > 0)

    def scale_copy(side):
        return pltpu.make_async_remote_copy(
            src_ref=scales.at[side],
            dst_ref=side_scales.at[side],
            send_sem=side_scale_sems.at[0, side],
            recv_sem=side_scale_sems.at[1, side],
            device_id={"row": sends[side][1]},
            device_id_type=mesh_type,
        )

    def side_copy(side, t):
        return pltpu.make_async_remote_copy(
            src_ref=codes.at[side, lax.rem(g + 1 + t, chunks)],
            dst_ref=side_codes.at[side, t],
            send_sem=side_sems.at[0, side, t],
            recv_sem=side_sems.at[1, side, t],
            device_id={"row": sends[side][1]},
            device_id_type=mesh_type,
        )

    def peer_copy(t):
        return pltpu.make_async_remote_copy(
            src_ref=sent_codes.at[t],
            dst_ref=peer_codes.at[t],
            send_sem=peer_sems.at[0, t],
            recv_sem=peer_sems.at[1, t],
            device_id={"grp": lax.rem(g + 1 + t, chunks)},
            device_id_type=mesh_type,
        )

    def peer_scale_copy(t):
        return pltpu.make_async_remote_copy(
            src_ref=sent_scales.at[t],
            dst_ref=peer_scales.at[t],
            send_sem=peer_scale_sems.at[0, t],
            recv_sem=peer_scale_sems.at[1, t],
            device_id={"grp": lax.rem(g + 1 + t, chunks)},
            device_id_type=mesh_type,
        )

    for side in range(2):

        @pl.when(sends[side][0])
        def _():
            scale_copy(side).start()
            for t in range(chunks):
                side_copy(side, t).start()

        @pl.when(jnp.logical_not(comes[side]))
        def _():
            side_scales[side] = jnp.zeros_like(side_scales[side])

            @pl.loop(0, chunks)
            def _(t):
                @pl.loop(0, members)
                def _(e):
                    side_codes[side, t, e] = jnp.zeros(side_codes.shape[3:], jnp.int16)

    for side in range(2):

        @pl.when(comes[side])
        def _():
            scale_copy(side).wait_recv()

    for t in range(chunks):
        d = lax.rem(g + 1 + t, chunks)
        for side in range(2):

            @pl.when(comes[side])
            def _():
                side_copy(side, t).wait_recv()

        @pl.loop(0, members)
        def _(e):
            value = center[d, e]
            for side in range(2):
                value += decoded(side_codes[side, t, e], side_scales[side, d, pl.ds(e, 1)])
            if t < chunks - 1:
                code, scale = encoded(value)
                sent_codes[t, e] = code
                sent_scales[t, pl.ds(e, 1)] = scale
            else:
                out[e] = value

        if t < chunks - 1:
            peer_scale_copy(t).start()
            peer_copy(t).start()

    for t in range(chunks - 1):
        peer_scale_copy(t).wait_recv()
        peer_copy(t).wait_recv()

        @pl.loop(0, members)
        def _(e):
            out[e] = out[e] + decoded(peer_codes[t, e], peer_scales[t, pl.ds(e, 1)])

    for t in range(chunks - 1):
        peer_scale_copy(t).wait_send()
        peer_copy(t).wait_send()
    for side in range(2):

        @pl.when(sends[side][0])
        def _():
            scale_copy(side).wait_send()
            for t in range(chunks):
                side_copy(side, t).wait_send()


def exchange(center, codes, scales, rows):
    chunks, members, tile, _ = center.shape
    vmem = pl.BlockSpec(memory_space=pltpu.VMEM)
    anywhere = pl.BlockSpec(memory_space=pl.ANY)
    dma = pltpu.SemaphoreType.DMA
    return pl.pallas_call(
        functools.partial(exchange_kernel, rows, chunks),
        out_shape=jax.ShapeDtypeStruct((members, tile, tile), jnp.float32),
        in_specs=[vmem, anywhere, vmem],
        out_specs=vmem,
        scratch_shapes=[
            pltpu.VMEM((2, chunks, members, tile, tile), jnp.int16),
            pltpu.VMEM((2, chunks, members, tile), jnp.float32),
            pltpu.VMEM((chunks - 1, members, tile, tile), jnp.int16),
            pltpu.VMEM((chunks - 1, members, tile), jnp.float32),
            pltpu.VMEM((chunks - 1, members, tile, tile), jnp.int16),
            pltpu.VMEM((chunks - 1, members, tile), jnp.float32),
            dma((2, 2, chunks)),
            dma((2, 2)),
            dma((2, chunks - 1)),
            dma((2, chunks - 1)),
        ],
        compiler_params=pltpu.CompilerParams(
            collective_id=0, has_side_effects=True, vmem_limit_bytes=40 * 1024 * 1024
        ),
    )(center, codes, scales)


def body(a_tiles, a_cols, p_tiles, p_cols, c_cols):
    fine_rows = a_tiles.shape[0]
    coarse_rows = fine_rows // RATIO
    tile = a_tiles.shape[-1]
    kc = c_cols.shape[1]
    chunks = lax.axis_size("grp")
    position = lax.axis_index("row")
    fetched = [passed_along(p_tiles, "row", offset) for offset in (2, 1, -1, -2)]
    band = jnp.concatenate([fetched[0], fetched[1], p_tiles, fetched[2], fetched[3]], axis=0)
    center, codes, scales = local_products(
        a_tiles, a_cols, band, p_cols, c_cols, position, chunks
    )
    out = exchange(center, codes, scales, lax.axis_size("row"))
    return out.reshape(coarse_rows, kc // chunks, tile, tile)


def solution(mesh):
    return jax.shard_map(
        body,
        mesh=mesh,
        in_specs=(
            P("row", "grp", None, None, None),
            P("row", "grp", None),
            P("row", None, None, None),
            P(),
            P(),
        ),
        out_specs=P("row", "grp", None, None),
        check_vma=False,
    )
```

```python
import functools

import jax
import jax.numpy as jnp
from jax import lax
from jax.experimental import pallas as pl
from jax.experimental.pallas import tpu as pltpu
from jax.sharding import PartitionSpec as P

RATIO = 2
REACH = 2


LEVELS = 32767.0


def encoded(value):
    most = jnp.maximum(jnp.max(jnp.abs(value), axis=0, keepdims=True), 2e-34)
    code = jnp.round(value * (LEVELS / most)).astype(jnp.int32).astype(jnp.int16)
    return code, most * (1.0 / LEVELS)


def decoded(code, scale):
    return code.astype(jnp.int32).astype(jnp.float32) * scale


def product_kernel(
    sizes,
    where,
    a_cols,
    p_cols,
    c_cols,
    a_ref,
    band_ref,
    center_ref,
    codes_ref,
    scales_ref,
    total_ref,
    spread,
    halves,
):
    fine_rows, slots, kp, kc, tile, chunks = sizes
    coarse_rows = fine_rows // RATIO
    window = (2 * (REACH + 1) + 1) * coarse_rows
    position = where[0]
    first_row = position * fine_rows
    band_start = first_row - REACH * fine_rows
    window_start = (position - REACH - 1) * coarse_rows
    base_coarse = (position - 1) * coarse_rows
    total_ref[...] = jnp.zeros_like(total_ref)
    halves[window] = jnp.zeros((2 * tile, tile), jnp.bfloat16)
    group = min(4, kc)

    @pl.loop(0, fine_rows)
    def _(i):
        spread[...] = jnp.zeros_like(spread)
        for s in range(slots):
            j = a_cols[i * slots + s]
            local = (j - band_start) * kp
            right = jnp.concatenate([band_ref[local + p] for p in range(kp)], axis=1)
            prod = jnp.dot(a_ref[i * slots + s], right, preferred_element_type=jnp.float32)
            for p in range(kp):
                w = p_cols[j * kp + p] - window_start
                spread[w] = spread[w] + prod[:, p * tile : (p + 1) * tile]

        @pl.loop(0, window, unroll=4)
        def _(w):
            value = spread[w]
            high = value.astype(jnp.bfloat16)
            halves[w, :tile] = high
            halves[w, tile:] = (value - high.astype(jnp.float32)).astype(jnp.bfloat16)

        for q in range(kp):
            c = p_cols[(first_row + i) * kp + q]
            own = band_ref[(REACH * fine_rows + i) * kp + q].T
            left = jnp.concatenate([own, own], axis=1)
            out = (c - base_coarse) * kc
            for k in range(0, kc, group):
                parts = []
                for n in range(group):
                    w = c_cols[c * kc + k + n] - window_start
                    w = jnp.where((w < 0) | (w >= window), window, w)
                    parts.append(halves[w])
                prod = jnp.dot(
                    left, jnp.concatenate(parts, axis=1), preferred_element_type=jnp.float32
                )
                for n in range(group):
                    at = out + k + n
                    total_ref[at] = total_ref[at] + prod[:, n * tile : (n + 1) * tile]

    share = kc // chunks
    for chunk in range(chunks):

        @pl.loop(0, coarse_rows)
        def _(c):
            for n in range(share):
                e = c * share + n
                k = chunk * share + n
                center_ref[chunk, e] = total_ref[(coarse_rows + c) * kc + k]
                for side in range(2):
                    value = total_ref[(2 * side * coarse_rows + c) * kc + k]
                    code, scale = encoded(value)
                    codes_ref[side, chunk, e] = code
                    scales_ref[side, chunk, pl.ds(e, 1)] = scale


def local_products(a_tiles, a_cols, band, p_cols, c_cols, position, chunks):
    fine_rows, _, slots, tile, _ = a_tiles.shape
    kp = band.shape[1]
    kc = c_cols.shape[1]
    coarse_rows = fine_rows // RATIO
    window = (2 * (REACH + 1) + 1) * coarse_rows
    members = coarse_rows * kc // chunks
    smem = pl.BlockSpec(memory_space=pltpu.SMEM)
    vmem = pl.BlockSpec(memory_space=pltpu.VMEM)
    return pl.pallas_call(
        functools.partial(product_kernel, (fine_rows, slots, kp, kc, tile, chunks)),
        out_shape=[
            jax.ShapeDtypeStruct((chunks, members, tile, tile), jnp.float32),
            jax.ShapeDtypeStruct((2, chunks, members, tile, tile), jnp.int16),
            jax.ShapeDtypeStruct((2, chunks, members, tile), jnp.float32),
        ],
        in_specs=[smem] * 4 + [vmem] * 2,
        out_specs=[vmem] * 3,
        scratch_shapes=[
            pltpu.VMEM((3 * coarse_rows * kc, tile, tile), jnp.float32),
            pltpu.VMEM((window, tile, tile), jnp.float32),
            pltpu.VMEM((window + 1, 2 * tile, tile), jnp.bfloat16),
        ],
        compiler_params=pltpu.CompilerParams(vmem_limit_bytes=56 * 1024 * 1024),
    )(
        position.reshape(1),
        a_cols.reshape(-1),
        p_cols.reshape(-1),
        c_cols.reshape(-1),
        a_tiles.reshape(-1, tile, tile),
        band.reshape(-1, tile, tile),
    )


def exchange_kernel(
    rows,
    chunks,
    center,
    codes,
    scales,
    out,
    side_codes,
    side_scales,
    sent_codes,
    sent_scales,
    peer_codes,
    peer_scales,
    side_sems,
    side_scale_sems,
    peer_sems,
    peer_scale_sems,
):
    r = lax.axis_index("row")
    g = lax.axis_index("grp")
    members = out.shape[0]
    barrier = pltpu.get_barrier_semaphore()
    mesh_type = pl.DeviceIdType.MESH

    def signal(where):
        pl.semaphore_signal(barrier, inc=1, device_id=where, device_id_type=mesh_type)

    for t in range(chunks - 1):
        signal({"grp": lax.rem(g + 1 + t, chunks)})

    @pl.when(r > 0)
    def _():
        signal({"row": r - 1})

    @pl.when(r < rows - 1)
    def _():
        signal({"row": r + 1})

    inside = (r > 0) & (r < rows - 1)

    @pl.when(inside)
    def _():
        pl.semaphore_wait(barrier, chunks + 1)

    @pl.when(jnp.logical_not(inside))
    def _():
        pl.semaphore_wait(barrier, chunks)

    sends = ((r > 0, r - 1), (r < rows - 1, r + 1))
    comes = (r < rows - 1, r > 0)

    def scale_copy(side):
        return pltpu.make_async_remote_copy(
            src_ref=scales.at[side],
            dst_ref=side_scales.at[side],
            send_sem=side_scale_sems.at[0, side],
            recv_sem=side_scale_sems.at[1, side],
            device_id={"row": sends[side][1]},
            device_id_type=mesh_type,
        )

    def side_copy(side, t):
        return pltpu.make_async_remote_copy(
            src_ref=codes.at[side, lax.rem(g + 1 + t, chunks)],
            dst_ref=side_codes.at[side, t],
            send_sem=side_sems.at[0, side, t],
            recv_sem=side_sems.at[1, side, t],
            device_id={"row": sends[side][1]},
            device_id_type=mesh_type,
        )

    def peer_copy(t):
        return pltpu.make_async_remote_copy(
            src_ref=sent_codes.at[t],
            dst_ref=peer_codes.at[t],
            send_sem=peer_sems.at[0, t],
            recv_sem=peer_sems.at[1, t],
            device_id={"grp": lax.rem(g + 1 + t, chunks)},
            device_id_type=mesh_type,
        )

    def peer_scale_copy(t):
        return pltpu.make_async_remote_copy(
            src_ref=sent_scales.at[t],
            dst_ref=peer_scales.at[t],
            send_sem=peer_scale_sems.at[0, t],
            recv_sem=peer_scale_sems.at[1, t],
            device_id={"grp": lax.rem(g + 1 + t, chunks)},
            device_id_type=mesh_type,
        )

    for side in range(2):

        @pl.when(sends[side][0])
        def _():
            scale_copy(side).start()
            for t in range(chunks):
                side_copy(side, t).start()

        @pl.when(jnp.logical_not(comes[side]))
        def _():
            side_scales[side] = jnp.zeros_like(side_scales[side])

            @pl.loop(0, chunks)
            def _(t):
                @pl.loop(0, members)
                def _(e):
                    side_codes[side, t, e] = jnp.zeros(side_codes.shape[3:], jnp.int16)

    for side in range(2):

        @pl.when(comes[side])
        def _():
            scale_copy(side).wait_recv()

    for t in range(chunks):
        d = lax.rem(g + 1 + t, chunks)
        for side in range(2):

            @pl.when(comes[side])
            def _():
                side_copy(side, t).wait_recv()

        @pl.loop(0, members)
        def _(e):
            value = center[d, e]
            for side in range(2):
                value += decoded(side_codes[side, t, e], side_scales[side, d, pl.ds(e, 1)])
            if t < chunks - 1:
                code, scale = encoded(value)
                sent_codes[t, e] = code
                sent_scales[t, pl.ds(e, 1)] = scale
            else:
                out[e] = value

        if t < chunks - 1:
            peer_scale_copy(t).start()
            peer_copy(t).start()

    for t in range(chunks - 1):
        peer_scale_copy(t).wait_recv()
        peer_copy(t).wait_recv()

        @pl.loop(0, members)
        def _(e):
            out[e] = out[e] + decoded(peer_codes[t, e], peer_scales[t, pl.ds(e, 1)])

    for t in range(chunks - 1):
        peer_scale_copy(t).wait_send()
        peer_copy(t).wait_send()
    for side in range(2):

        @pl.when(sends[side][0])
        def _():
            scale_copy(side).wait_send()
            for t in range(chunks):
                side_copy(side, t).wait_send()


def exchange(center, codes, scales, rows):
    chunks, members, tile, _ = center.shape
    vmem = pl.BlockSpec(memory_space=pltpu.VMEM)
    anywhere = pl.BlockSpec(memory_space=pl.ANY)
    dma = pltpu.SemaphoreType.DMA
    return pl.pallas_call(
        functools.partial(exchange_kernel, rows, chunks),
        out_shape=jax.ShapeDtypeStruct((members, tile, tile), jnp.float32),
        in_specs=[vmem, anywhere, vmem],
        out_specs=vmem,
        scratch_shapes=[
            pltpu.VMEM((2, chunks, members, tile, tile), jnp.int16),
            pltpu.VMEM((2, chunks, members, tile), jnp.float32),
            pltpu.VMEM((chunks - 1, members, tile, tile), jnp.int16),
            pltpu.VMEM((chunks - 1, members, tile), jnp.float32),
            pltpu.VMEM((chunks - 1, members, tile, tile), jnp.int16),
            pltpu.VMEM((chunks - 1, members, tile), jnp.float32),
            dma((2, 2, chunks)),
            dma((2, 2)),
            dma((2, chunks - 1)),
            dma((2, chunks - 1)),
        ],
        compiler_params=pltpu.CompilerParams(
            collective_id=0, has_side_effects=True, vmem_limit_bytes=40 * 1024 * 1024
        ),
    )(center, codes, scales)


def gather_kernel(rows, pieces, own, band, up_sems, down_sems, pair_sems, pass_sems, own_sem):
    r = lax.axis_index("row")
    odd = lax.rem(r, 2)
    partner = r + 1 - 2 * odd
    has_down = r >= 2
    has_up = r < rows - 2
    step = own.shape[0] // pieces
    barrier = pltpu.get_barrier_semaphore()
    mesh_type = pl.DeviceIdType.MESH

    def copy(src, dst, sems, c, to):
        return pltpu.make_async_remote_copy(
            src_ref=src,
            dst_ref=dst,
            send_sem=sems.at[0, c],
            recv_sem=sems.at[1, c],
            device_id={"row": to},
            device_id_type=mesh_type,
        )

    def part(c):
        return pl.ds(c * step, step)

    def up(c):
        return copy(own.at[part(c)], band.at[0, part(c)], up_sems, c, r + 2)

    def down(c):
        return copy(own.at[part(c)], band.at[4, part(c)], down_sems, c, r - 2)

    def pair():
        return copy(own, band.at[1 + 2 * odd], pair_sems, 0, partner)

    def passed(c):
        return copy(
            band.at[4 - 4 * odd, part(c)], band.at[3 - 2 * odd, part(c)], pass_sems, c, partner
        )

    def signal(to):
        pl.semaphore_signal(barrier, inc=1, device_id={"row": to}, device_id_type=mesh_type)

    signal(partner)
    pl.when(has_up)(lambda: signal(r + 2))
    pl.when(has_down)(lambda: signal(r - 2))
    pl.when(has_up & has_down)(lambda: pl.semaphore_wait(barrier, 3))
    pl.when(jnp.logical_not(has_up & has_down))(lambda: pl.semaphore_wait(barrier, 2))

    for c in range(pieces):
        pl.when(has_up)(lambda: up(c).start())
        pl.when(has_down)(lambda: down(c).start())
    pair().start()
    local = pltpu.make_async_copy(own, band.at[2], own_sem)
    local.start()

    @pl.when((odd == 0) & has_up)
    def _():
        for c in range(pieces):
            down(c).wait_recv()
            passed(c).start()

    @pl.when((odd == 1) & has_down)
    def _():
        for c in range(pieces):
            up(c).wait_recv()
            passed(c).start()

    @pl.when((odd == 0) & has_down)
    def _():
        for c in range(pieces):
            up(c).wait_recv()
            passed(c).wait_recv()

    @pl.when((odd == 1) & has_up)
    def _():
        for c in range(pieces):
            down(c).wait_recv()
            passed(c).wait_recv()

    local.wait()
    pair().wait_recv()
    pair().wait_send()
    for c in range(pieces):
        pl.when(has_up)(lambda: up(c).wait_send())
        pl.when(has_down)(lambda: down(c).wait_send())

    @pl.when(((odd == 0) & has_up) | ((odd == 1) & has_down))
    def _():
        for c in range(pieces):
            passed(c).wait_send()


def gathered(p_tiles, rows):
    fine_rows = p_tiles.shape[0]
    pieces = min(8, fine_rows)
    vmem = pl.BlockSpec(memory_space=pltpu.VMEM)
    dma = pltpu.SemaphoreType.DMA
    return pl.pallas_call(
        functools.partial(gather_kernel, rows, pieces),
        out_shape=jax.ShapeDtypeStruct((5,) + p_tiles.shape, p_tiles.dtype),
        in_specs=[vmem],
        out_specs=vmem,
        scratch_shapes=[dma((2, pieces))] * 2 + [dma((2, 1)), dma((2, pieces)), dma],
        compiler_params=pltpu.CompilerParams(
            collective_id=1, has_side_effects=True, vmem_limit_bytes=16 * 1024 * 1024
        ),
    )(p_tiles)


def body(a_tiles, a_cols, p_tiles, p_cols, c_cols):
    fine_rows = a_tiles.shape[0]
    coarse_rows = fine_rows // RATIO
    tile = a_tiles.shape[-1]
    kc = c_cols.shape[1]
    chunks = lax.axis_size("grp")
    position = lax.axis_index("row")
    band = gathered(p_tiles, lax.axis_size("row"))
    band = band.reshape((5 * fine_rows,) + p_tiles.shape[1:])
    center, codes, scales = local_products(
        a_tiles, a_cols, band, p_cols, c_cols, position, chunks
    )
    out = exchange(center, codes, scales, lax.axis_size("row"))
    return out.reshape(coarse_rows, kc // chunks, tile, tile)


def solution(mesh):
    return jax.shard_map(
        body,
        mesh=mesh,
        in_specs=(
            P("row", "grp", None, None, None),
            P("row", "grp", None),
            P("row", None, None, None),
            P(),
            P(),
        ),
        out_specs=P("row", "grp", None, None),
        check_vma=False,
    )
```
